128 devices in a mesh: dp: 16 (over x, y), mp: 8 (over z, core).
Axes of the slice: x: 4, y: 4, z: 4, core: 2. Of those that a mesh axis runs over, the one named last changes fastest.
Arguments:
- activations: bfloat16 [16384, 4096], P(('dp', 'mp')), may hold values from -17 to 17
- output_grads: bfloat16 [16384, 14336], P('dp', 'mp'), may hold values from -0.046875 to 0.046875
- q_start: float32 [14336, 64], P('mp'), may hold values from -6 to 6
Outputs:
- new_error: bfloat16 [65536, 14336], P('dp', 'mp')
- q_factor: float32 [14336, 64], P('mp')
The draws below stay inside these ranges and needn't reach their ends.
All inputs are finite; a program needn't handle non-finite values.
Results may differ from the reference program's by a relative error of at most 0.01.
Values may be sent and summed in bfloat16 or wider, within the bound.
A program may use at most 192 MiB of HBM per device.

```python
import jax
import jax.numpy as jnp
from jax import lax

D = 4096
FF = 14336
R = 64
TOK_REP = 1024
TOKENS = 16384
N_DP = 16


def draw_activations(key, part):
    key_base = jax.random.fold_in(key, 11)
    key_cols = jax.random.fold_in(key, 12)
    column = jnp.arange(D, dtype=jnp.float32) / D
    ramp = jnp.exp(jnp.log(3.0) * (column - 0.5))
    rough = jnp.exp(jax.random.uniform(key_cols, (D,), jnp.float32, -1.15, 1.15))
    scales = ramp * rough / 1.3
    base = jax.random.normal(key_base, (TOKENS, D), jnp.float32)
    base = jnp.clip(base, -4.0, 4.0)
    return (base * scales[None, :]).astype(jnp.bfloat16)


def shard_levels(rng, dims, split, least, largest):
    factor_of = 1.0
    for position, shards_of in split:
        draws = jax.random.uniform(jax.random.fold_in(jax.random.fold_in(rng, 6), position), (shards_of,), jnp.float32, least / len(split), largest / len(split))
        factor_of = factor_of * jnp.repeat(jnp.exp(draws), dims[position] // shards_of).reshape((-1,) + (1,) * (len(dims) - 1 - position))
    return factor_of


def normal_values(rng, shape, width, most, pieces=(), kind=jnp.bfloat16):
    array = width * jax.random.normal(rng, shape, jnp.float32)
    if pieces:
        array = array * shard_levels(rng, shape, pieces, -0.22, 0.18)
    return jnp.clip(array, -most, most).astype(kind)


def setup_inputs(seed: int = 0) -> dict:
    seeds = jax.random.split(jax.random.key(seed), 4)
    activations = draw_activations(jax.random.fold_in(seeds[3], 71), 0)
    output_grads = normal_values(seeds[1], (TOKENS, FF), (16 * TOK_REP) ** -0.5, 0.046875, ((0, 16), (1, 8)))
    q_start = normal_values(seeds[2], (FF, R), 1.0, 6.0, ((0, 8),), jnp.float32)
    return {"activations": activations, "output_grads": output_grads, "q_start": q_start}


def reference(activations, output_grads, q_start):
    highest = lax.Precision.HIGHEST
    inputs_rep = activations.reshape(N_DP, TOK_REP, D)
    grads_rep = output_grads.reshape(N_DP, TOK_REP, FF)

    def left_step(carry, pair):
        inputs, grads = pair
        projected = jnp.dot(grads.astype(jnp.float32), q_start, precision=highest)
        return (carry + jnp.dot(inputs.astype(jnp.float32).T, projected, precision=highest), None)
    p_summed, unused = lax.scan(left_step, jnp.zeros((D, R), jnp.float32), (inputs_rep, grads_rep))
    p_mean = p_summed / N_DP
    gram_matrix = jnp.dot(p_mean.T, p_mean, precision=highest)
    lower_tri = jnp.linalg.cholesky(gram_matrix)
    p_ortho = lax.linalg.triangular_solve(lower_tri, p_mean, left_side=False, lower=True, transpose_a=True)

    def right_step(carry, pair):
        inputs, grads = pair
        gradient = jnp.dot(inputs.T.astype(jnp.float32), grads.astype(jnp.float32), preferred_element_type=jnp.float32)
        return (carry + jnp.dot(gradient.T, p_ortho, precision=highest), None)
    q_summed, unused_two = lax.scan(right_step, jnp.zeros((FF, R), jnp.float32), (inputs_rep, grads_rep))
    q_factor = q_summed / N_DP
    decompressed = jnp.dot(p_ortho, q_factor.T, precision=highest)

    def error_one(pair):
        inputs, grads = pair
        gradient = jnp.dot(inputs.T.astype(jnp.float32), grads.astype(jnp.float32), preferred_element_type=jnp.float32)
        return (gradient - decompressed).astype(jnp.bfloat16)
    errors = lax.map(error_one, (inputs_rep, grads_rep))
    return (errors.reshape(N_DP * D, FF), q_factor)
```

```python
import jax
import jax.numpy as jnp
from jax import lax
from jax.experimental import pallas as pl
from jax.experimental.pallas import tpu as pltpu
from jax.sharding import PartitionSpec as P

MESH = pl.DeviceIdType.MESH
BF, F32 = jnp.bfloat16, jnp.float32
D, FFL, R, TOK = 4096, 1792, 64, 1024
BLK, NB = 128, 32
CB = 14
ROWS = 1024
NN = (((1,), (0,)), ((), ()))
NT = (((1,), (1,)), ((), ()))
TN = (((0,), (0,)), ((), ()))


def dot(a, b, dims=NN):
    return lax.dot_general(a, b, dims, preferred_element_type=F32)


def halves(v):
    upper = v.astype(BF)
    return upper, (v - upper.astype(F32)).astype(BF)


def dot3(a, b, dims=NN):
    (ah, al), (bh, bl) = halves(a), halves(b)
    return dot(ah, bh, dims) + (dot(ah, bl, dims) + dot(al, bh, dims))


def factor_kernel(
    x_hbm, y_hbm, q_hbm, g0, g1, g2, g3, p_out, q_out, c_out,
    x_v, y_v, q_v, xt, af, a_s, a_r, pown, pc_s, pc_r, px_s, px_r, py_f, py_s, py_r, pz, pt,
    xpb, qf, qs, qx_r, qy_f, qy_s, qy_r, qa, linv,
    ld_sem, a_ss, a_rs, c_ss, c_rs, x_ss, x_rs, y_ss, y_rs, z_ss, z_rs,
    gy_ss, gy_rs, gx_ss, gx_rs, gc_ss, gc_rs, xp_ss, xp_rs,
    qx_ss, qx_rs, qy_ss, qy_rs, hy_ss, hy_rs, hx_ss, hx_rs,
    own_s, own_r, up_s, up_r, dn_s, dn_r, fw_s, fw_r, pf_s, pf_r,
):
    g_refs = (g0, g1, g2, g3)
    r, m = lax.axis_index("dp"), lax.axis_index("mp")
    x, y = r // 4, lax.rem(r, 4)
    z, c = m // 2, lax.rem(m, 2)
    partner = {"dp": r, "mp": z * 2 + (1 - c)}

    def mp_peer(k):
        return {"dp": r, "mp": lax.rem(m + k, 8)}

    def x_peer(k):
        return {"dp": lax.rem(x + k, 4) * 4 + y, "mp": m}

    def y_peer(k):
        return {"dp": x * 4 + lax.rem(y + k, 4), "mp": m}

    def z_peer(k):
        return {"dp": r, "mp": lax.rem(z + k, 4) * 2 + c}

    sent = []

    def push(src, dst, ssem, rsem, dev):
        cp = pltpu.make_async_remote_copy(
            src_ref=src, dst_ref=dst, send_sem=ssem, recv_sem=rsem, device_id=dev, device_id_type=MESH
        )
        cp.start()
        sent.append(cp)
        return cp

    x_cp = pltpu.make_async_copy(x_hbm, x_v, ld_sem.at[0])
    q_cp = pltpu.make_async_copy(q_hbm, q_v, ld_sem.at[1])
    y_cps = [
        pltpu.make_async_copy(y_hbm.at[pl.ds(256 * i, 256)], y_v.at[pl.ds(256 * i, 256)], ld_sem.at[2 + i])
        for i in range(4)
    ]
    x_cp.start()
    q_cp.start()
    for cp in y_cps:
        cp.start()

    bar = pltpu.get_barrier_semaphore()
    for dev in [mp_peer(k) for k in range(1, 8)] + [f(k) for f in (x_peer, y_peer) for k in (1, 2, 3)]:
        pl.semaphore_signal(bar, inc=1, device_id=dev, device_id_type=MESH)

    x_cp.wait()
    for i in range(4):
        xt[m, 1024 * i : 1024 * (i + 1), :] = x_v[:, 1024 * i : 1024 * (i + 1)].T

    pl.semaphore_wait(bar, 13)
    own = push(xt.at[m], xt.at[m], own_s.at[0], own_r.at[0], partner)

    q_cp.wait()
    qh, ql = halves(q_v[...])
    qq = jnp.concatenate([qh, ql], axis=0)
    for i in range(4):
        y_cps[i].wait()
        both = dot(qq, y_v[256 * i : 256 * (i + 1), :], NT)
        at = both[:R] + both[R:]
        for h in range(2):
            blk = at[:, BLK * h : BLK * (h + 1)]
            af[2 * i + h] = blk
            a_s[2 * i + h] = blk.astype(BF)
    a_cps = []
    for k in range(1, 8):
        to = lax.rem(m + k, 8)
        a_cps.append(push(a_s.at[to], a_r.at[k - 1], a_ss.at[k - 1], a_rs.at[k - 1], mp_peer(k)))

    def rows(j):
        return pl.ds(ROWS * j, ROWS)

    def ring_own(j_up, j_dn):
        u = push(xt.at[m, rows(j_up)], xt.at[m, rows(j_up)], up_s.at[j_up], up_r.at[j_up], z_peer(1))
        d = push(xt.at[m, rows(j_dn)], xt.at[m, rows(j_dn)], dn_s.at[j_dn], dn_r.at[j_dn], z_peer(3))
        return {("u", j_up): u, ("d", j_dn): d}

    ring = {}
    ring.update(ring_own(0, 2))
    ring.update(ring_own(1, 3))

    def g_tile(zz, j, first):
        def body(h, carry):
            at_row = pl.multiple_of(512 * h, 512)
            src = pl.multiple_of(ROWS * j + 512 * h, 512)
            lhs = jnp.concatenate([xt[2 * zz, pl.ds(src, 512), :], xt[2 * zz + 1, pl.ds(src, 512), :]], axis=1)
            for n in range(7):
                w = y_v[pl.ds(pl.multiple_of(256 * zz, 256), 256), 256 * n : 256 * (n + 1)]
                prod = dot(lhs, w)
                spot = (pl.ds(at_row, 512), slice(256 * n, 256 * (n + 1)))
                if first:
                    g_refs[j][spot] = prod
                else:
                    g_refs[j][spot] = g_refs[j][spot] + prod
            return carry

        lax.fori_loop(0, 2, body, 0)

    own.wait_recv()
    for j in range(4):
        g_tile(z, j, True)

    at = af[m]
    for k in range(1, 8):
        a_cps[k - 1].wait_recv()
    for k in range(1, 8):
        at = at + a_r[k - 1].astype(F32)

    ath, atl = halves(at)
    aa = jnp.concatenate([ath, atl], axis=0)

    def p_part(half, write):
        for b in range(8):
            col = pl.multiple_of(half * 2048 + 256 * b, 256)
            both = dot(aa, x_v[:, pl.ds(col, 256)])
            s = both[:R] + both[R:]
            write(2 * b, s[:, :BLK])
            write(2 * b + 1, s[:, BLK:])

    def put_send(b, v):
        pc_s[b] = v.astype(BF)

    def put_own(b, v):
        pown[b] = v

    p_part(1 - c, put_send)
    pc = push(pc_s, pc_r, c_ss.at[0], c_rs.at[0], partner)
    p_part(c, put_own)
    pc.wait_recv()
    tot = pown[...] + pc_r[...].astype(F32)
    pown[...] = tot
    px_s[...] = tot.astype(BF)
    cps = []
    for k in (1, 2, 3):
        to = lax.rem(x + k, 4)
        cps.append(push(px_s.at[pl.ds(4 * to, 4)], px_r.at[k - 1], x_ss.at[k - 1], x_rs.at[k - 1], x_peer(k)))
    tot = pown[pl.ds(4 * x, 4)]
    for k in (1, 2, 3):
        cps[k - 1].wait_recv()
        tot = tot + px_r[k - 1].astype(F32)
    py_f[...] = tot
    py_s[...] = tot.astype(BF)
    cps = []
    for k in (1, 2, 3):
        to = lax.rem(y + k, 4)
        cps.append(push(py_s.at[to], py_r.at[k - 1], y_ss.at[k - 1], y_rs.at[k - 1], y_peer(k)))
    tot = py_f[y]
    for k in (1, 2, 3):
        cps[k - 1].wait_recv()
        tot = tot + py_r[k - 1].astype(F32)
    pz[z] = tot * (1.0 / 16.0)
    cps = [push(pz.at[z], pz.at[z], z_ss.at[k - 1], z_rs.at[k - 1], z_peer(k)) for k in (1, 2, 3)]
    ring.update(ring_own(2, 0))
    ring.update(ring_own(3, 1))
    for cp in cps:
        cp.wait_recv()
    blk = c * 16 + x * 4 + y
    pt[blk] = ((pz[0] + pz[1]) + (pz[2] + pz[3])).astype(BF)

    cps = [push(pt.at[blk], pt.at[blk], gy_ss.at[k - 1], gy_rs.at[k - 1], y_peer(k)) for k in (1, 2, 3)]
    for cp in cps:
        cp.wait_recv()

    def quad(xx):
        return pt.at[pl.ds(c * 16 + 4 * xx, 4)]

    cps = [push(quad(x), quad(x), gx_ss.at[k - 1], gx_rs.at[k - 1], x_peer(k)) for k in (1, 2, 3)]
    pcs = [push(quad(x), quad(x), gc_ss.at[0], gc_rs.at[0], partner)]
    for k in (1, 2, 3):
        cps[k - 1].wait_recv()
        src = quad(lax.rem(x + 4 - k, 4))
        pcs.append(push(src, src, gc_ss.at[k], gc_rs.at[k], partner))
    for cp in pcs:
        cp.wait_recv()

    acc = jnp.zeros((R, BLK), F32)
    for b in range(16):
        acc = acc + dot(jnp.concatenate([pt[2 * b], pt[2 * b + 1]], axis=1), xt[m, 256 * b : 256 * (b + 1), :])
    xpb[m] = acc.astype(BF)
    xp_cps = [push(xpb.at[m], xpb.at[m], xp_ss.at[k - 1], xp_rs.at[k - 1], mp_peer(k)) for k in range(1, 8)]

    below, above, across = lax.rem(z + 3, 4), lax.rem(z + 1, 4), lax.rem(z + 2, 4)
    pfs = []

    def hand_over(owner, j, idx):
        at_ = xt.at[2 * owner + c, rows(j)]
        pfs.append(push(at_, at_, pf_s.at[idx], pf_r.at[idx], partner))

    fwd = []
    for i in range(2):
        ring[("u", i)].wait_recv()
        s = xt.at[2 * below + c, rows(i)]
        fwd.append(push(s, s, fw_s.at[i], fw_r.at[i], z_peer(1)))
        ring[("d", 2 + i)].wait_recv()
        s = xt.at[2 * above + c, rows(2 + i)]
        fwd.append(push(s, s, fw_s.at[2 + i], fw_r.at[2 + i], z_peer(3)))
        hand_over(below, i, i)
        hand_over(above, 2 + i, 4 + 2 + i)

    gram = jnp.zeros((R, R), F32)
    for b in range(16):
        pp = jnp.concatenate([pt[2 * b], pt[2 * b + 1]], axis=1)
        gram = gram + dot(pp, pp, NT)

    for cp in xp_cps:
        cp.wait_recv()

    xpt = jnp.concatenate([xpb[i] for i in range(8)], axis=1)
    for n in range(7):
        part = dot(xpt, y_v[:, 256 * n : 256 * (n + 1)]) * (1.0 / 16.0)
        for h in range(2):
            for i in range(4):
                v = part[16 * i : 16 * (i + 1), BLK * h : BLK * (h + 1)]
                qf[i, 2 * n + h] = v
                qs[i, 2 * n + h] = v.astype(BF)
    cps = []
    for k in (1, 2, 3):
        to = lax.rem(x + k, 4)
        cps.append(push(qs.at[to], qx_r.at[k - 1], qx_ss.at[k - 1], qx_rs.at[k - 1], x_peer(k)))

    lane = lax.broadcasted_iota(jnp.int32, (R, 2 * R), 1)
    row = lax.broadcasted_iota(jnp.int32, (R, 2 * R), 0)
    eye = jnp.where(lane == row + R, 1.0, 0.0)
    work = jnp.concatenate([gram, jnp.zeros((R, R), F32)], axis=1) + eye

    def eliminate(j, w):
        rj = jnp.sum(jnp.where(row == j, w, 0.0), axis=0, keepdims=True)
        cj = jnp.sum(jnp.where(lane == j, w, 0.0), axis=1, keepdims=True)
        dj = jnp.sum(jnp.where(lane[:1] == j, rj, 0.0), axis=1, keepdims=True)
        f = jnp.where(row[:, :1] > j, cj / dj, 0.0)
        return w - f * rj

    work = lax.fori_loop(0, R, eliminate, work)
    diag = jnp.sum(jnp.where(lane == row, work, 0.0), axis=1, keepdims=True)
    linv[...] = work[:, R:] / jnp.sqrt(diag)

    tot = qf[x]
    for k in (1, 2, 3):
        cps[k - 1].wait_recv()
        tot = tot + qx_r[k - 1].astype(F32)
    qy_f[0:CB] = tot
    qy_f[CB:16] = jnp.zeros((2, 16, BLK), F32)
    qy_s[0:CB] = tot.astype(BF)
    qy_s[CB:16] = jnp.zeros((2, 16, BLK), BF)
    cps = []
    for k in (1, 2, 3):
        to = lax.rem(y + k, 4)
        cps.append(push(qy_s.at[pl.ds(4 * to, 4)], qy_r.at[k - 1], qy_ss.at[k - 1], qy_rs.at[k - 1], y_peer(k)))

    for i in range(2):
        ring[("u", 2 + i)].wait_recv()
        ring[("d", i)].wait_recv()
        hand_over(below, 2 + i, 2 + i)
        hand_over(above, i, 4 + i)

    tot = qy_f[pl.ds(4 * y, 4)]
    for k in (1, 2, 3):
        cps[k - 1].wait_recv()
        tot = tot + qy_r[k - 1].astype(F32)

    def mine(yy):
        return qa.at[x, pl.ds(4 * yy, 4)]

    qa[x, pl.ds(4 * y, 4)] = tot
    cps = [push(mine(y), mine(y), hy_ss.at[k - 1], hy_rs.at[k - 1], y_peer(k)) for k in (1, 2, 3)]

    for cp in pfs[:]:
        cp.wait_recv()
    for j in range(4):
        g_tile(below, j, False)

    for cp in cps:
        cp.wait_recv()
    cps = [push(qa.at[x], qa.at[x], hx_ss.at[k - 1], hx_rs.at[k - 1], x_peer(k)) for k in (1, 2, 3)]
    for j in range(4):
        g_tile(above, j, False)
    last = []
    for i in range(2):
        fwd[2 * i].wait_recv()
        fwd[2 * i + 1].wait_recv()
        hand_over(across, i, 8 + i)
        hand_over(across, 2 + i, 8 + 2 + i)
    for cp in cps:
        cp.wait_recv()

    li = linv[...]
    for b in range(7):
        raw = jnp.concatenate(
            [jnp.concatenate([qa[i, 2 * b + h] for i in range(4)], axis=0) for h in range(2)], axis=1
        )
        qt = dot3(li, raw)
        q_out[:, 256 * b : 256 * (b + 1)] = qt
        c_out[:, 256 * b : 256 * (b + 1)] = dot3(li, qt, TN).astype(BF)
    for b in range(NB):
        p_out[BLK * b : BLK * (b + 1), :] = pt[b].T

    for cp in pfs[8:]:
        cp.wait_recv()
    for j in range(4):
        g_tile(across, j, False)
    for cp in sent:
        cp.wait_send()


def finish_kernel(g0, g1, g2, g3, p_ref, q_ref, c_ref, e_ref, q_out):
    i = pl.program_id(0)
    q_out[...] = q_ref[...]
    at_row = pl.multiple_of(lax.rem(i, 2) * 512, 512)
    for s, g in enumerate((g0, g1, g2, g3)):

        @pl.when(i // 2 == s)
        def _(g=g):
            p = p_ref[pl.ds(pl.multiple_of(i * 512, 512), 512), :]
            for n in range(7):
                cols = slice(256 * n, 256 * (n + 1))
                e_ref[:, cols] = (g[pl.ds(at_row, 512), cols] - dot(p, c_ref[:, cols])).astype(BF)


def per_device(activations, output_grads, q_start):
    vm = pl.BlockSpec(memory_space=pltpu.VMEM)
    dma = pltpu.SemaphoreType.DMA
    outs = pl.pallas_call(
        factor_kernel,
        out_shape=[jax.ShapeDtypeStruct((ROWS, FFL), F32)] * 4
        + [
            jax.ShapeDtypeStruct((D, R), BF),
            jax.ShapeDtypeStruct((R, FFL), F32),
            jax.ShapeDtypeStruct((R, FFL), BF),
        ],
        in_specs=[pl.BlockSpec(memory_space=pl.ANY)] * 3,
        out_specs=[vm] * 7,
        scratch_shapes=[
            pltpu.VMEM((128, D), BF),
            pltpu.VMEM((TOK, FFL), BF),
            pltpu.VMEM((R, FFL), F32),
            pltpu.VMEM((8, D, 128), BF),
            pltpu.VMEM((8, R, BLK), F32),
            pltpu.VMEM((8, R, BLK), BF),
            pltpu.VMEM((7, R, BLK), BF),
            pltpu.VMEM((16, R, BLK), F32),
            pltpu.VMEM((16, R, BLK), BF),
            pltpu.VMEM((16, R, BLK), BF),
            pltpu.VMEM((16, R, BLK), BF),
            pltpu.VMEM((3, 4, R, BLK), BF),
            pltpu.VMEM((4, R, BLK), F32),
            pltpu.VMEM((4, R, BLK), BF),
            pltpu.VMEM((3, R, BLK), BF),
            pltpu.VMEM((4, R, BLK), F32),
            pltpu.VMEM((NB, R, BLK), BF),
            pltpu.VMEM((8, R, BLK), BF),
            pltpu.VMEM((4, CB, 16, BLK), F32),
            pltpu.VMEM((4, CB, 16, BLK), BF),
            pltpu.VMEM((3, CB, 16, BLK), BF),
            pltpu.VMEM((16, 16, BLK), F32),
            pltpu.VMEM((16, 16, BLK), BF),
            pltpu.VMEM((3, 4, 16, BLK), BF),
            pltpu.VMEM((4, 16, 16, BLK), F32),
            pltpu.VMEM((R, R), F32),
            dma((6,)),
            dma((7,)), dma((7,)),
            dma((1,)), dma((1,)),
            dma((3,)), dma((3,)),
            dma((3,)), dma((3,)),
            dma((3,)), dma((3,)),
            dma((3,)), dma((3,)),
            dma((3,)), dma((3,)),
            dma((4,)), dma((4,)),
            dma((7,)), dma((7,)),
            dma((3,)), dma((3,)),
            dma((3,)), dma((3,)),
            dma((3,)), dma((3,)),
            dma((3,)), dma((3,)),
            dma((1,)), dma((1,)),
            dma((4,)), dma((4,)),
            dma((4,)), dma((4,)),
            dma((4,)), dma((4,)),
            dma((12,)), dma((12,)),
        ],
        compiler_params=pltpu.CompilerParams(collective_id=0, has_side_effects=True, vmem_limit_bytes=20 * 2**20),
        name="factors",
    )(
        pltpu.with_memory_space_constraint(activations, pltpu.HBM),
        pltpu.with_memory_space_constraint(output_grads, pltpu.HBM),
        pltpu.with_memory_space_constraint(q_start.T, pltpu.HBM),
    )
    new_error, q_factor = pl.pallas_call(
        finish_kernel,
        grid=(8,),
        out_shape=(jax.ShapeDtypeStruct((D, FFL), BF), jax.ShapeDtypeStruct((R, FFL), F32)),
        in_specs=[vm] * 7,
        out_specs=(pl.BlockSpec((512, FFL), lambda i: (i, 0)), pl.BlockSpec((R, FFL), lambda i: (0, 0))),
        compiler_params=pltpu.CompilerParams(vmem_limit_bytes=12 * 2**20),
        name="finish",
    )(*outs)
    return new_error, q_factor.T


def solution(mesh):
    in_specs = (P(("dp", "mp"), None), P("dp", "mp"), P("mp", None))
    out_specs = (P("dp", "mp"), P("mp", None))
    return jax.shard_map(per_device, mesh=mesh, in_specs=in_specs, out_specs=out_specs, check_vma=False)
```

```python
import jax
import jax.numpy as jnp
from jax import lax
from jax.experimental import pallas as pl
from jax.experimental.pallas import tpu as pltpu
from jax.sharding import PartitionSpec as P

MESH = pl.DeviceIdType.MESH
BF, F32 = jnp.bfloat16, jnp.float32
D, FFL, R, TOK = 4096, 1792, 64, 1024
BLK, NB = 128, 32
ROWS = 1024
FAR_FIRST = sorted(range(1, 16), key=lambda o: -(min(o // 4, 4 - o // 4) + min(o % 4, 4 - o % 4)))
NN = (((1,), (0,)), ((), ()))
NT = (((1,), (1,)), ((), ()))
TN = (((0,), (0,)), ((), ()))


def dot(a, b, dims=NN):
    return lax.dot_general(a, b, dims, preferred_element_type=F32)


def halves(v):
    upper = v.astype(BF)
    return upper, (v - upper.astype(F32)).astype(BF)


def dot3(a, b, dims=NN):
    (ah, al), (bh, bl) = halves(a), halves(b)
    return dot(ah, bh, dims) + (dot(ah, bl, dims) + dot(al, bh, dims))


def factor_kernel(
    x_hbm, y_hbm, q_hbm, g0, g1, g2, g3, p_out, q_out, c_out,
    x_v, y_v, q_v, xt, af, a_s, a_r, pown, pc_s, pc_r, px_s, px_r, pz, pt, xpb, qf, qs, q_r, qa, linv,
    ld_sem, a_ss, a_rs, c_ss, c_rs, p_ss, p_rs, z_ss, z_rs, gp_ss, gp_rs, gc_ss, gc_rs, xp_ss, xp_rs,
    q_ss, q_rs, gq_ss, gq_rs, own_s, own_r, up_s, up_r, dn_s, dn_r, fw_s, fw_r, pf_s, pf_r,
):
    g_refs = (g0, g1, g2, g3)
    r, m = lax.axis_index("dp"), lax.axis_index("mp")
    z, c = m // 2, lax.rem(m, 2)
    partner = {"dp": r, "mp": z * 2 + (1 - c)}

    def mp_peer(k):
        return {"dp": r, "mp": lax.rem(m + k, 8)}

    def dp_peer(k):
        return {"dp": lax.rem(r + k, 16), "mp": m}

    def z_peer(k):
        return {"dp": r, "mp": lax.rem(z + k, 4) * 2 + c}

    sent = []

    def push(src, dst, ssem, rsem, dev):
        cp = pltpu.make_async_remote_copy(
            src_ref=src, dst_ref=dst, send_sem=ssem, recv_sem=rsem, device_id=dev, device_id_type=MESH
        )
        cp.start()
        sent.append(cp)
        return cp

    q_cp = pltpu.make_async_copy(q_hbm, q_v, ld_sem.at[1])
    x_cp = pltpu.make_async_copy(x_hbm, x_v, ld_sem.at[0])
    y_cps = [
        pltpu.make_async_copy(y_hbm.at[pl.ds(256 * i, 256)], y_v.at[pl.ds(256 * i, 256)], ld_sem.at[2 + i])
        for i in range(4)
    ]
    q_cp.start()
    for cp in y_cps:
        cp.start()
    x_cp.start()

    bar = pltpu.get_barrier_semaphore()
    for dev in [mp_peer(k) for k in range(1, 8)] + [dp_peer(k) for k in range(1, 16)]:
        pl.semaphore_signal(bar, inc=1, device_id=dev, device_id_type=MESH)

    q_cp.wait()
    qh, ql = halves(q_v[...])
    qq = jnp.concatenate([qh, ql], axis=0)
    for i in range(4):
        y_cps[i].wait()
        both = dot(qq, y_v[256 * i : 256 * (i + 1), :], NT)
        at = both[:R] + both[R:]
        for h in range(2):
            blk = at[:, BLK * h : BLK * (h + 1)]
            af[2 * i + h] = blk
            a_s[2 * i + h] = blk.astype(BF)
    pl.semaphore_wait(bar, 22)
    a_cps = []
    for k in (4, 3, 5, 2, 6, 1, 7):
        to = lax.rem(m + k, 8)
        a_cps.append(push(a_s.at[to], a_r.at[k - 1], a_ss.at[k - 1], a_rs.at[k - 1], mp_peer(k)))

    x_cp.wait()
    for i in range(4):
        xt[m, 1024 * i : 1024 * (i + 1), :] = x_v[:, 1024 * i : 1024 * (i + 1)].T
    own = push(xt.at[m], xt.at[m], own_s.at[0], own_r.at[0], partner)

    def rows(j):
        return pl.ds(ROWS * j, ROWS)

    ring = {}

    def ring_own(i):
        for key, j, ss, rs, k in (("u", i, up_s, up_r, 1), ("d", (i + 2) % 4, dn_s, dn_r, 3)):
            here = xt.at[m, rows(j)]
            ring[key, j] = push(here, here, ss.at[j], rs.at[j], z_peer(k))

    below, above, across = lax.rem(z + 3, 4), lax.rem(z + 1, 4), lax.rem(z + 2, 4)
    pfs = {}

    def hand_over(name, owner, j, idx):
        here = xt.at[2 * owner + c, rows(j)]
        pfs[name, j] = push(here, here, pf_s.at[idx], pf_r.at[idx], partner)

    def arrived(i):
        j = (i + 2) % 4
        ring["u", i].wait_recv()
        hand_over("below", below, i, i)
        ring["d", j].wait_recv()
        hand_over("above", above, j, 4 + j)

    fwd = {}

    def forward(i):
        j = i + 2
        here = xt.at[2 * below + c, rows(i)]
        fwd[i] = push(here, here, fw_s.at[i], fw_r.at[i], z_peer(1))
        here = xt.at[2 * above + c, rows(j)]
        fwd[j] = push(here, here, fw_s.at[j], fw_r.at[j], z_peer(3))

    def arrived_far(i):
        for j in (i, i + 2):
            fwd[j].wait_recv()
            hand_over("across", across, j, 8 + j)

    ring_own(0)
    ring_own(1)

    def g_tile(zz, j, first=False):
        def body(h, carry):
            at_row = pl.multiple_of(512 * h, 512)
            src = pl.multiple_of(ROWS * j + 512 * h, 512)
            lhs = jnp.concatenate([xt[2 * zz, pl.ds(src, 512), :], xt[2 * zz + 1, pl.ds(src, 512), :]], axis=1)
            for n in range(7):
                w = y_v[pl.ds(pl.multiple_of(256 * zz, 256), 256), 256 * n : 256 * (n + 1)]
                prod = dot(lhs, w)
                spot = (pl.ds(at_row, 512), slice(256 * n, 256 * (n + 1)))
                if first:
                    g_refs[j][spot] = prod
                else:
                    g_refs[j][spot] = g_refs[j][spot] + prod
            return carry

        lax.fori_loop(0, 2, body, 0)

    def g_far(name, zz, j):
        pfs[name, j].wait_recv()
        g_tile(zz, j)

    at = af[m]
    for cp in a_cps:
        cp.wait_recv()
    for k in range(1, 8):
        at = at + a_r[k - 1].astype(F32)

    ath, atl = halves(at)
    aa = jnp.concatenate([ath, atl], axis=0)

    def p_part(half, write):
        for b in range(8):
            col = pl.multiple_of(half * 2048 + 256 * b, 256)
            both = dot(aa, x_v[:, pl.ds(col, 256)])
            s = both[:R] + both[R:]
            write(2 * b, s[:, :BLK])
            write(2 * b + 1, s[:, BLK:])

    def put_send(b, v):
        pc_s[b] = v.astype(BF)

    def put_own(b, v):
        pown[b] = v

    p_part(1 - c, put_send)
    pc = push(pc_s, pc_r, c_ss.at[0], c_rs.at[0], partner)
    p_part(c, put_own)
    own.wait_recv()
    g_tile(z, 0, True)
    pc.wait_recv()
    tot = pown[...] + pc_r[...].astype(F32)
    pown[...] = tot
    px_s[...] = tot.astype(BF)
    cps = []
    for k in FAR_FIRST:
        to = lax.rem(r + k, 16)
        cps.append(push(px_s.at[to], px_r.at[k - 1], p_ss.at[k - 1], p_rs.at[k - 1], dp_peer(k)))
    for j in range(1, 4):
        g_tile(z, j, True)
    arrived(0)
    for cp in cps:
        cp.wait_recv()
    tot = pown[r]
    for k in range(1, 16):
        tot = tot + px_r[k - 1].astype(F32)
    pz[z] = tot * (1.0 / 16.0)
    cps = [push(pz.at[z], pz.at[z], z_ss.at[k - 1], z_rs.at[k - 1], z_peer(k)) for k in (2, 1, 3)]
    ring_own(2)
    g_far("below", below, 0)
    g_far("above", above, 2)
    for cp in cps:
        cp.wait_recv()
    blk = c * 16 + r
    pt[blk] = ((pz[0] + pz[1]) + (pz[2] + pz[3])).astype(BF)

    cps = [(k, push(pt.at[blk], pt.at[blk], gp_ss.at[k - 1], gp_rs.at[k - 1], dp_peer(k))) for k in FAR_FIRST]
    pcs = [push(pt.at[blk], pt.at[blk], gc_ss.at[0], gc_rs.at[0], partner)]
    ring_own(3)
    arrived(1)
    g_far("below", below, 1)
    g_far("above", above, 3)
    for k, cp in reversed(cps):
        cp.wait_recv()
        here = pt.at[c * 16 + lax.rem(r + 16 - k, 16)]
        pcs.append(push(here, here, gc_ss.at[k], gc_rs.at[k], partner))
    for cp in pcs:
        cp.wait_recv()

    acc = jnp.zeros((R, BLK), F32)
    for b in range(16):
        acc = acc + dot(jnp.concatenate([pt[2 * b], pt[2 * b + 1]], axis=1), xt[m, 256 * b : 256 * (b + 1), :])
    xpb[m] = acc.astype(BF)
    xp_cps = [push(xpb.at[m], xpb.at[m], xp_ss.at[k - 1], xp_rs.at[k - 1], mp_peer(k)) for k in (4, 3, 5, 2, 6, 1, 7)]
    forward(0)
    forward(1)
    arrived(2)

    gram = jnp.zeros((R, R), F32)
    for b in range(16):
        pp = jnp.concatenate([pt[2 * b], pt[2 * b + 1]], axis=1)
        gram = gram + dot(pp, pp, NT)
    g_far("below", below, 2)
    g_far("above", above, 0)

    for cp in xp_cps:
        cp.wait_recv()

    xpt = jnp.concatenate([xpb[i] for i in range(8)], axis=1)
    for i in range(4):
        qs[4 * i + 3, 2:4] = jnp.zeros((2, 16, BLK), BF)
        qf[4 * i + 3, 2:4] = jnp.zeros((2, 16, BLK), F32)
    for n in range(7):
        part = dot(xpt, y_v[:, 256 * n : 256 * (n + 1)]) * (1.0 / 16.0)
        for h in range(2):
            cb = 2 * n + h
            for i in range(4):
                v = part[16 * i : 16 * (i + 1), BLK * h : BLK * (h + 1)]
                qf[4 * i + cb // 4, cb % 4] = v
                qs[4 * i + cb // 4, cb % 4] = v.astype(BF)
    cps = []
    for k in FAR_FIRST:
        to = lax.rem(r + k, 16)
        cps.append(push(qs.at[to], q_r.at[k - 1], q_ss.at[k - 1], q_rs.at[k - 1], dp_peer(k)))
    arrived(3)

    lane = lax.broadcasted_iota(jnp.int32, (R, 2 * R), 1)
    row = lax.broadcasted_iota(jnp.int32, (R, 2 * R), 0)
    eye = jnp.where(lane == row + R, 1.0, 0.0)
    work = jnp.concatenate([gram, jnp.zeros((R, R), F32)], axis=1) + eye

    def eliminate(j, w):
        rj = jnp.sum(jnp.where(row == j, w, 0.0), axis=0, keepdims=True)
        cj = jnp.sum(jnp.where(lane == j, w, 0.0), axis=1, keepdims=True)
        dj = jnp.sum(jnp.where(lane[:1] == j, rj, 0.0), axis=1, keepdims=True)
        f = jnp.where(row[:, :1] > j, cj / dj, 0.0)
        return w - f * rj

    work = lax.fori_loop(0, R, eliminate, work)
    diag = jnp.sum(jnp.where(lane == row, work, 0.0), axis=1, keepdims=True)
    linv[...] = work[:, R:] / jnp.sqrt(diag)

    for cp in cps:
        cp.wait_recv()
    tot = qf[r]
    for k in range(1, 16):
        tot = tot + q_r[k - 1].astype(F32)
    qa[r] = tot.astype(BF)
    cps = [push(qa.at[r], qa.at[r], gq_ss.at[k - 1], gq_rs.at[k - 1], dp_peer(k)) for k in FAR_FIRST]

    g_far("below", below, 3)
    g_far("above", above, 1)
    arrived_far(0)
    for b in range(NB):
        p_out[BLK * b : BLK * (b + 1), :] = pt[b].T
    g_far("across", across, 0)
    g_far("across", across, 2)
    arrived_far(1)
    for cp in cps:
        cp.wait_recv()

    lh, ll = halves(linv[...])
    for b in range(7):
        raw = jnp.concatenate(
            [
                jnp.concatenate([qa[4 * i + cb // 4, cb % 4] for i in range(4)], axis=0)
                for cb in (2 * b, 2 * b + 1)
            ],
            axis=1,
        )
        qt = dot(lh, raw) + dot(ll, raw)
        q_out[:, 256 * b : 256 * (b + 1)] = qt
        c_out[:, 256 * b : 256 * (b + 1)] = dot3(linv[...], qt, TN).astype(BF)

    g_far("across", across, 1)
    g_far("across", across, 3)
    for cp in sent:
        cp.wait_send()


def finish_kernel(g0, g1, g2, g3, p_ref, q_ref, c_ref, e_ref, q_out):
    i = pl.program_id(0)
    q_out[...] = q_ref[...]
    at_row = pl.multiple_of(lax.rem(i, 2) * 512, 512)
    for s, g in enumerate((g0, g1, g2, g3)):

        @pl.when(i // 2 == s)
        def _(g=g):
            p = p_ref[pl.ds(pl.multiple_of(i * 512, 512), 512), :]
            for n in range(7):
                cols = slice(256 * n, 256 * (n + 1))
                e_ref[:, cols] = (g[pl.ds(at_row, 512), cols] - dot(p, c_ref[:, cols])).astype(BF)


def per_device(activations, output_grads, q_start):
    vm = pl.BlockSpec(memory_space=pltpu.VMEM)
    dma = pltpu.SemaphoreType.DMA
    outs = pl.pallas_call(
        factor_kernel,
        out_shape=[jax.ShapeDtypeStruct((ROWS, FFL), F32)] * 4
        + [
            jax.ShapeDtypeStruct((D, R), BF),
            jax.ShapeDtypeStruct((R, FFL), F32),
            jax.ShapeDtypeStruct((R, FFL), BF),
        ],
        in_specs=[pl.BlockSpec(memory_space=pl.ANY)] * 3,
        out_specs=[vm] * 7,
        scratch_shapes=[
            pltpu.VMEM((128, D), BF),
            pltpu.VMEM((TOK, FFL), BF),
            pltpu.VMEM((R, FFL), F32),
            pltpu.VMEM((8, D, 128), BF),
            pltpu.VMEM((8, R, BLK), F32),
            pltpu.VMEM((8, R, BLK), BF),
            pltpu.VMEM((7, R, BLK), BF),
            pltpu.VMEM((16, R, BLK), F32),
            pltpu.VMEM((16, R, BLK), BF),
            pltpu.VMEM((16, R, BLK), BF),
            pltpu.VMEM((16, R, BLK), BF),
            pltpu.VMEM((15, R, BLK), BF),
            pltpu.VMEM((4, R, BLK), F32),
            pltpu.VMEM((NB, R, BLK), BF),
            pltpu.VMEM((8, R, BLK), BF),
            pltpu.VMEM((16, 4, 16, BLK), F32),
            pltpu.VMEM((16, 4, 16, BLK), BF),
            pltpu.VMEM((15, 4, 16, BLK), BF),
            pltpu.VMEM((16, 4, 16, BLK), BF),
            pltpu.VMEM((R, R), F32),
            dma((6,)),
            dma((7,)), dma((7,)),
            dma((1,)), dma((1,)),
            dma((15,)), dma((15,)),
            dma((3,)), dma((3,)),
            dma((15,)), dma((15,)),
            dma((16,)), dma((16,)),
            dma((7,)), dma((7,)),
            dma((15,)), dma((15,)),
            dma((15,)), dma((15,)),
            dma((1,)), dma((1,)),
            dma((4,)), dma((4,)),
            dma((4,)), dma((4,)),
            dma((4,)), dma((4,)),
            dma((12,)), dma((12,)),
        ],
        compiler_params=pltpu.CompilerParams(collective_id=0, has_side_effects=True, vmem_limit_bytes=20 * 2**20),
        name="factors",
    )(
        pltpu.with_memory_space_constraint(activations, pltpu.HBM),
        pltpu.with_memory_space_constraint(output_grads, pltpu.HBM),
        pltpu.with_memory_space_constraint(q_start.T, pltpu.HBM),
    )
    new_error, q_factor = pl.pallas_call(
        finish_kernel,
        grid=(8,),
        out_shape=(jax.ShapeDtypeStruct((D, FFL), BF), jax.ShapeDtypeStruct((R, FFL), F32)),
        in_specs=[vm] * 7,
        out_specs=(pl.BlockSpec((512, FFL), lambda i: (i, 0)), pl.BlockSpec((R, FFL), lambda i: (0, 0))),
        compiler_params=pltpu.CompilerParams(vmem_limit_bytes=12 * 2**20),
        name="finish",
    )(*outs)
    return new_error, q_factor.T


def solution(mesh):
    in_specs = (P(("dp", "mp"), None), P("dp", "mp"), P("mp", None))
    out_specs = (P("dp", "mp"), P("mp", None))
    return jax.shard_map(per_device, mesh=mesh, in_specs=in_specs, out_specs=out_specs, check_vma=False)
```

```python
import jax
import jax.numpy as jnp
from jax import lax
from jax.experimental import pallas as pl
from jax.experimental.pallas import tpu as pltpu
from jax.sharding import PartitionSpec as P

MESH = pl.DeviceIdType.MESH
BF, F32 = jnp.bfloat16, jnp.float32
D, FFL, R, TOK = 4096, 1792, 64, 1024
BLK, NB = 128, 32
ROWS = 1024
PIECES = 8
FAR_FIRST = sorted(range(1, 16), key=lambda o: -(min(o // 4, 4 - o // 4) + min(o % 4, 4 - o % 4)))
NN = (((1,), (0,)), ((), ()))
NT = (((1,), (1,)), ((), ()))
TN = (((0,), (0,)), ((), ()))


def dot(a, b, dims=NN):
    return lax.dot_general(a, b, dims, preferred_element_type=F32)


def halves(v):
    upper = v.astype(BF)
    return upper, (v - upper.astype(F32)).astype(BF)


def dot3(a, b, dims=NN):
    (ah, al), (bh, bl) = halves(a), halves(b)
    return dot(ah, bh, dims) + (dot(ah, bl, dims) + dot(al, bh, dims))


def factor_kernel(
    x_hbm, y_hbm, q_hbm, g0, g1, g2, g3, p_out, q_out, c_out,
    x_v, y_v, q_v, xt, af, a_s, a_r, pown, pc_s, pc_r, px_s, px_r, pz, pt, xpb, qf, qs, q_r, qa, linv,
    ld_sem, a_ss, a_rs, c_ss, c_rs, p_ss, p_rs, z_ss, z_rs, gp_ss, gp_rs, gc_ss, gc_rs, xp_ss, xp_rs,
    q_ss, q_rs, gq_ss, gq_rs, own_s, own_r, up_s, up_r, dn_s, dn_r, fw_s, fw_r, pf_s, pf_r,
):
    g_refs = (g0, g1, g2, g3)
    r, m = lax.axis_index("dp"), lax.axis_index("mp")
    z, c = m // 2, lax.rem(m, 2)
    partner = {"dp": r, "mp": z * 2 + (1 - c)}

    def mp_peer(k):
        return {"dp": r, "mp": lax.rem(m + k, 8)}

    def dp_peer(k):
        return {"dp": lax.rem(r + k, 16), "mp": m}

    def z_peer(k):
        return {"dp": r, "mp": lax.rem(z + k, 4) * 2 + c}

    sent = []

    def push(src, dst, ssem, rsem, dev):
        cp = pltpu.make_async_remote_copy(
            src_ref=src, dst_ref=dst, send_sem=ssem, recv_sem=rsem, device_id=dev, device_id_type=MESH
        )
        cp.start()
        sent.append(cp)
        return cp

    q_cp = pltpu.make_async_copy(q_hbm, q_v, ld_sem.at[1])
    x_cp = pltpu.make_async_copy(x_hbm, x_v, ld_sem.at[0])
    y_cps = [
        pltpu.make_async_copy(y_hbm.at[pl.ds(256 * i, 256)], y_v.at[pl.ds(256 * i, 256)], ld_sem.at[2 + i])
        for i in range(4)
    ]
    x_cp.start()
    q_cp.start()
    for cp in y_cps:
        cp.start()

    bar = pltpu.get_barrier_semaphore()
    for dev in [mp_peer(k) for k in range(1, 8)] + [dp_peer(k) for k in range(1, 16)]:
        pl.semaphore_signal(bar, inc=1, device_id=dev, device_id_type=MESH)

    x_cp.wait()
    for i in range(4):
        xt[m, 1024 * i : 1024 * (i + 1), :] = x_v[:, 1024 * i : 1024 * (i + 1)].T

    def rows(j):
        return pl.ds(ROWS * j, ROWS)

    ring = {}

    def ring_own(i):
        for key, j, ss, rs, k in (("u", i, up_s, up_r, 1), ("d", (i + 2) % 4, dn_s, dn_r, 3)):
            here = xt.at[m, rows(j)]
            ring[key, j] = push(here, here, ss.at[j], rs.at[j], z_peer(k))

    below, above, across = lax.rem(z + 3, 4), lax.rem(z + 1, 4), lax.rem(z + 2, 4)
    pfs = {}

    def hand_over(name, owner, j, idx):
        here = xt.at[2 * owner + c, rows(j)]
        pfs[name, j] = push(here, here, pf_s.at[idx], pf_r.at[idx], partner)

    def arrived(i):
        j = (i + 2) % 4
        ring["u", i].wait_recv()
        ring["d", j].wait_recv()
        hand_over("below", below, i, i)
        hand_over("above", above, j, 4 + j)

    fwd = {}

    def forward(i):
        j = i + 2
        here = xt.at[2 * below + c, rows(i)]
        fwd[i] = push(here, here, fw_s.at[i], fw_r.at[i], z_peer(1))
        here = xt.at[2 * above + c, rows(j)]
        fwd[j] = push(here, here, fw_s.at[j], fw_r.at[j], z_peer(3))

    def arrived_far(i):
        for j in (i, i + 2):
            fwd[j].wait_recv()
            hand_over("across", across, j, 8 + j)

    q_cp.wait()
    qh, ql = halves(q_v[...])
    qq = jnp.concatenate([qh, ql], axis=0)
    for first, count in ((0, 2), (2, 6)):
        for cp in y_cps[first // 2 : (first + count) // 2]:
            cp.wait()
        both = dot(qq, y_v[BLK * first : BLK * (first + count), :], NT)
        at = both[:R] + both[R:]
        for h in range(count):
            blk = at[:, BLK * h : BLK * (h + 1)]
            af[first + h] = blk
            a_s[first + h] = blk.astype(BF)
    pl.semaphore_wait(bar, 22)
    a_cps = []
    for k in (4, 3, 5, 2, 6, 1, 7):
        to = lax.rem(m + k, 8)
        a_cps.append(push(a_s.at[to], a_r.at[k - 1], a_ss.at[k - 1], a_rs.at[k - 1], mp_peer(k)))

    own = push(xt.at[m], xt.at[m], own_s.at[0], own_r.at[0], partner)
    ring_own(0)
    ring_own(1)

    def g_tile(zz, j, first=False):
        w_rows = pl.ds(pl.multiple_of(256 * zz, 256), 256)

        def part(here, there):
            lhs = jnp.concatenate([xt[2 * zz, here, :], xt[2 * zz + 1, here, :]], axis=1)
            for n in range(7):
                cols = slice(256 * n, 256 * (n + 1))
                prod = dot(lhs, y_v[w_rows, cols])
                g_refs[j][there, cols] = prod if first else g_refs[j][there, cols] + prod

        if first:
            part(rows(j), slice(None))
            return

        def body(h, carry):
            at_row = pl.multiple_of(512 * h, 512)
            part(pl.ds(pl.multiple_of(ROWS * j + at_row, 512), 512), pl.ds(at_row, 512))
            return carry

        lax.fori_loop(0, 2, body, 0)

    def g_far(name, zz, j):
        pfs[name, j].wait_recv()
        g_tile(zz, j)

    at = af[m]
    for cp in a_cps:
        cp.wait_recv()
    for k in range(1, 8):
        at = at + a_r[k - 1].astype(F32)

    ath, atl = halves(at)
    aa = jnp.concatenate([ath, atl], axis=0)

    def p_part(half, write):
        for b in range(8):
            col = pl.multiple_of(half * 2048 + 256 * b, 256)
            both = dot(aa, x_v[:, pl.ds(col, 256)])
            s = both[:R] + both[R:]
            write(2 * b, s[:, :BLK])
            write(2 * b + 1, s[:, BLK:])

    def put_send(b, v):
        pc_s[b] = v.astype(BF)

    def put_own(b, v):
        pown[b] = v

    p_part(1 - c, put_send)
    pc = push(pc_s, pc_r, c_ss.at[0], c_rs.at[0], partner)
    p_part(c, put_own)
    own.wait_recv()
    g_tile(z, 0, True)
    pc.wait_recv()
    tot = pown[...] + pc_r[...].astype(F32)
    pown[...] = tot
    px_s[...] = tot.astype(BF)
    cps = []
    for k in FAR_FIRST:
        to = lax.rem(r + k, 16)
        cps.append(push(px_s.at[to], px_r.at[k - 1], p_ss.at[k - 1], p_rs.at[k - 1], dp_peer(k)))
    for j in range(1, 4):
        g_tile(z, j, True)
    arrived(0)
    for cp in cps:
        cp.wait_recv()
    tot = pown[r]
    for k in range(1, 16):
        tot = tot + px_r[k - 1].astype(F32)
    pz[z] = tot * (1.0 / 16.0)
    cps = [push(pz.at[z], pz.at[z], z_ss.at[k - 1], z_rs.at[k - 1], z_peer(k)) for k in (2, 1, 3)]
    ring_own(2)
    g_far("below", below, 0)
    g_far("above", above, 2)
    arrived(1)
    for cp in cps:
        cp.wait_recv()
    blk = c * 16 + r
    pt[blk] = ((pz[0] + pz[1]) + (pz[2] + pz[3])).astype(BF)

    cps = [(k, push(pt.at[blk], pt.at[blk], gp_ss.at[k - 1], gp_rs.at[k - 1], dp_peer(k))) for k in FAR_FIRST]
    pcs = [push(pt.at[blk], pt.at[blk], gc_ss.at[0], gc_rs.at[0], partner)]
    ring_own(3)
    g_far("below", below, 1)
    g_far("above", above, 3)
    for k, cp in reversed(cps):
        cp.wait_recv()
        here = pt.at[c * 16 + lax.rem(r + 16 - k, 16)]
        pcs.append(push(here, here, gc_ss.at[k], gc_rs.at[k], partner))
    for cp in pcs:
        cp.wait_recv()

    acc = jnp.zeros((R, BLK), F32)
    for b in range(16):
        acc = acc + dot(jnp.concatenate([pt[2 * b], pt[2 * b + 1]], axis=1), xt[m, 256 * b : 256 * (b + 1), :])
    xpb[m] = acc.astype(BF)
    xp_cps = [push(xpb.at[m], xpb.at[m], xp_ss.at[k - 1], xp_rs.at[k - 1], mp_peer(k)) for k in (4, 3, 5, 2, 6, 1, 7)]
    forward(0)
    forward(1)

    gram = jnp.zeros((R, R), F32)
    for b in range(16):
        pp = jnp.concatenate([pt[2 * b], pt[2 * b + 1]], axis=1)
        gram = gram + dot(pp, pp, NT)
    arrived(2)
    lane = lax.broadcasted_iota(jnp.int32, (R, 2 * R), 1)
    row = lax.broadcasted_iota(jnp.int32, (R, 2 * R), 0)
    eye = jnp.where(lane == row + R, 1.0, 0.0)
    work = jnp.concatenate([gram, jnp.zeros((R, R), F32)], axis=1) + eye

    def eliminate(i, w):
        j = 2 * i
        r1 = jnp.sum(jnp.where(row == j, w, 0.0), axis=0, keepdims=True)
        r2 = jnp.sum(jnp.where(row == j + 1, w, 0.0), axis=0, keepdims=True)
        c1 = jnp.sum(jnp.where(lane == j, w, 0.0), axis=1, keepdims=True)
        c2 = jnp.sum(jnp.where(lane == j + 1, w, 0.0), axis=1, keepdims=True)
        da = jnp.sum(jnp.where(lane[:1] == j, r1, 0.0), axis=1, keepdims=True)
        db = jnp.sum(jnp.where(lane[:1] == j + 1, r1, 0.0), axis=1, keepdims=True)
        dc = jnp.sum(jnp.where(lane[:1] == j + 1, r2, 0.0), axis=1, keepdims=True)
        inv = 1.0 / da
        ratio = db * inv
        f2 = (c2 - ratio * c1) / (dc - ratio * db)
        f1 = (c1 - db * f2) * inv
        f1 = jnp.where(row[:, :1] > j + 1, f1, jnp.where(row[:, :1] == j + 1, ratio, 0.0))
        f2 = jnp.where(row[:, :1] > j + 1, f2, 0.0)
        return w - (f1 * r1 + f2 * r2)

    work = lax.fori_loop(0, R // 2, eliminate, work)
    diag = jnp.sum(jnp.where(lane == row, work, 0.0), axis=1, keepdims=True)
    linv[...] = work[:, R:] / jnp.sqrt(diag)

    arrived(3)
    for cp in xp_cps:
        cp.wait_recv()

    xpt = jnp.concatenate([xpb[i] for i in range(8)], axis=1)
    for i in range(4):
        qs[4 * i + 3, 2:4] = jnp.zeros((2, 16, BLK), BF)
        qf[4 * i + 3, 2:4] = jnp.zeros((2, 16, BLK), F32)
    for n in range(7):
        part = dot(xpt, y_v[:, 256 * n : 256 * (n + 1)]) * (1.0 / 16.0)
        for h in range(2):
            cb = 2 * n + h
            for i in range(4):
                v = part[16 * i : 16 * (i + 1), BLK * h : BLK * (h + 1)]
                qf[4 * i + cb // 4, cb % 4] = v
                qs[4 * i + cb // 4, cb % 4] = v.astype(BF)
    cps = []
    for k in FAR_FIRST:
        to = lax.rem(r + k, 16)
        cps.append(push(qs.at[to], q_r.at[k - 1], q_ss.at[k - 1], q_rs.at[k - 1], dp_peer(k)))
    g_far("below", below, 2)
    g_far("above", above, 0)
    g_far("below", below, 3)
    arrived_far(0)
    g_far("above", above, 1)
    for cp in cps:
        cp.wait_recv()
    tot = qf[r]
    for k in range(1, 16):
        tot = tot + q_r[k - 1].astype(F32)
    qa[r] = tot.astype(BF)
    cps = [push(qa.at[r], qa.at[r], gq_ss.at[k - 1], gq_rs.at[k - 1], dp_peer(k)) for k in FAR_FIRST]

    g_far("across", across, 0)
    g_far("across", across, 2)
    arrived_far(1)
    for b in range(NB):
        p_out[BLK * b : BLK * (b + 1), :] = pt[b].T
    g_far("across", across, 1)
    g_far("across", across, 3)
    for cp in cps:
        cp.wait_recv()

    lh, ll = halves(linv[...])
    for b in range(7):
        raw = jnp.concatenate(
            [
                jnp.concatenate([qa[4 * i + cb // 4, cb % 4] for i in range(4)], axis=0)
                for cb in (2 * b, 2 * b + 1)
            ],
            axis=1,
        )
        qt = dot(lh, raw) + dot(ll, raw)
        q_out[:, 256 * b : 256 * (b + 1)] = qt
        c_out[:, 256 * b : 256 * (b + 1)] = dot3(linv[...], qt, TN).astype(BF)

    for cp in sent:
        cp.wait_send()


def finish_kernel(g0, g1, g2, g3, p_ref, q_ref, c_ref, e_hbm, q_hbm, e_v, sem):
    q_cp = pltpu.make_async_copy(q_ref, q_hbm, sem.at[0])
    q_cp.start()
    cps = [q_cp]
    for i in range(PIECES):
        here = slice(D // PIECES * i, D // PIECES * (i + 1))
        g = (g0, g1, g2, g3)[D // PIECES * i // ROWS]
        base = D // PIECES * i % ROWS
        p = p_ref[here, :]
        for n in range(7):
            cols = slice(256 * n, 256 * (n + 1))
            e_v[here, cols] = (g[base : base + D // PIECES, cols] - dot(p, c_ref[:, cols])).astype(BF)
        cps.append(pltpu.make_async_copy(e_v.at[here], e_hbm.at[here], sem.at[1 + i]))
        cps[-1].start()
    for cp in cps:
        cp.wait()


def per_device(activations, output_grads, q_start):
    vm = pl.BlockSpec(memory_space=pltpu.VMEM)
    dma = pltpu.SemaphoreType.DMA
    outs = pl.pallas_call(
        factor_kernel,
        out_shape=[jax.ShapeDtypeStruct((ROWS, FFL), F32)] * 4
        + [
            jax.ShapeDtypeStruct((D, R), BF),
            jax.ShapeDtypeStruct((R, FFL), F32),
            jax.ShapeDtypeStruct((R, FFL), BF),
        ],
        in_specs=[pl.BlockSpec(memory_space=pl.ANY)] * 3,
        out_specs=[vm] * 7,
        scratch_shapes=[
            pltpu.VMEM((128, D), BF),
            pltpu.VMEM((TOK, FFL), BF),
            pltpu.VMEM((R, FFL), F32),
            pltpu.VMEM((8, D, 128), BF),
            pltpu.VMEM((8, R, BLK), F32),
            pltpu.VMEM((8, R, BLK), BF),
            pltpu.VMEM((7, R, BLK), BF),
            pltpu.VMEM((16, R, BLK), F32),
            pltpu.VMEM((16, R, BLK), BF),
            pltpu.VMEM((16, R, BLK), BF),
            pltpu.VMEM((16, R, BLK), BF),
            pltpu.VMEM((15, R, BLK), BF),
            pltpu.VMEM((4, R, BLK), F32),
            pltpu.VMEM((NB, R, BLK), BF),
            pltpu.VMEM((8, R, BLK), BF),
            pltpu.VMEM((16, 4, 16, BLK), F32),
            pltpu.VMEM((16, 4, 16, BLK), BF),
            pltpu.VMEM((15, 4, 16, BLK), BF),
            pltpu.VMEM((16, 4, 16, BLK), BF),
            pltpu.VMEM((R, R), F32),
            dma((6,)),
            dma((7,)), dma((7,)),
            dma((1,)), dma((1,)),
            dma((15,)), dma((15,)),
            dma((3,)), dma((3,)),
            dma((15,)), dma((15,)),
            dma((16,)), dma((16,)),
            dma((7,)), dma((7,)),
            dma((15,)), dma((15,)),
            dma((15,)), dma((15,)),
            dma((1,)), dma((1,)),
            dma((4,)), dma((4,)),
            dma((4,)), dma((4,)),
            dma((4,)), dma((4,)),
            dma((12,)), dma((12,)),
        ],
        compiler_params=pltpu.CompilerParams(collective_id=0, has_side_effects=True, vmem_limit_bytes=20 * 2**20),
        name="factors",
    )(
        pltpu.with_memory_space_constraint(activations, pltpu.HBM),
        pltpu.with_memory_space_constraint(output_grads, pltpu.HBM),
        pltpu.with_memory_space_constraint(q_start.T, pltpu.HBM),
    )
    new_error, q_factor = pl.pallas_call(
        finish_kernel,
        out_shape=(jax.ShapeDtypeStruct((D, FFL), BF), jax.ShapeDtypeStruct((R, FFL), F32)),
        in_specs=[vm] * 7,
        out_specs=(pl.BlockSpec(memory_space=pl.ANY), pl.BlockSpec(memory_space=pl.ANY)),
        scratch_shapes=[pltpu.VMEM((D, FFL), BF), dma((1 + PIECES,))],
        compiler_params=pltpu.CompilerParams(vmem_limit_bytes=17 * 2**20),
        name="finish",
    )(*outs)
    return new_error, q_factor.T


def solution(mesh):
    in_specs = (P(("dp", "mp"), None), P("dp", "mp"), P("mp", None))
    out_specs = (P("dp", "mp"), P("mp", None))
    return jax.shard_map(per_device, mesh=mesh, in_specs=in_specs, out_specs=out_specs, check_vma=False)
```
